32 devices in a mesh: seq: 4 (over z), uly: 4 (over y, x), rep: 2 (over core).
Axes of the slice: x: 2, y: 2, z: 4, core: 2. Of those that a mesh axis runs over, the one named last changes fastest.
Arguments:
- queries: bfloat16 [4096, 2048], P(('rep', 'seq', 'uly')), parts along dimension 0, may hold values from -6 to 6
- keys: bfloat16 [4096, 2048], P(('rep', 'seq', 'uly')), parts along dimension 0, may hold values from -6 to 6
- values: bfloat16 [4096, 2048], P(('rep', 'seq', 'uly')), parts along dimension 0, may hold values from -6 to 6
- past_outputs: bfloat16 [2, 4096, 2048], P(None, ('rep', 'seq', 'uly')), parts along dimension 1, may hold values from -6 to 6
- dwa_slot: int32 [2], replicated, may hold values from 0 to 63
- dwa_table: float32 [2, 64], replicated, may hold values from 0.1 to 0.6
Outputs:
- mixed: bfloat16 [4096, 2048], P(('rep', 'seq', 'uly')), parts along dimension 0
The draws below stay inside these ranges and needn't reach their ends.
There are 2 independent parts, one for each index of `rep`. The reference program is written for one: setup_inputs(seed, part) draws one part's arguments, and reference() takes and returns one part's arrays. A program takes and returns all parts, laid end to end along the dimension named above; an argument that names none is the same for every part. Nothing has to cross between parts.
All inputs are finite; a program needn't handle non-finite values.
Results may differ from the reference program's by a relative error of at most 0.0034.
Values may be sent and summed in bfloat16 or wider, within the bound.
A program may use at most 64 MiB of HBM per device.

```python
import jax
import jax.numpy as jnp
from jax import lax

HEADS = 16
HEAD_DIM = 128
PAST = 2
TABLE = 64
TOK_DEV = 128
SPAN = 4
TOKENS = 2048
N_SEQ = 4
N_ULY = 4


def drawn_pair(key):
    base = jax.random.fold_in(key, 7)
    width = HEADS * HEAD_DIM
    query_field = jnp.clip(2.5 * jax.random.normal(jax.random.fold_in(base, 1), (TOKENS, width), jnp.float32), -6.0, 6.0)
    key_field = jnp.clip(jax.random.normal(jax.random.fold_in(base, 2), (TOKENS, width), jnp.float32), -6.0, 6.0)
    return (query_field, key_field)


def draw_queries(key, part):
    return drawn_pair(key)[0].astype(jnp.bfloat16)


def draw_keys(key, part):
    return drawn_pair(key)[1].astype(jnp.bfloat16)


def block_levels(rng, shape, split, low, largest):
    factor_of, own = 1.0, jax.random.fold_in(rng, 6)
    for dim, shards_of in split:
        heights = jnp.exp(jax.random.uniform(jax.random.fold_in(own, dim), (shards_of,), jnp.float32, low / len(split), largest / len(split)))
        factor_of = factor_of * jnp.repeat(heights, shape[dim] // shards_of).reshape([-1 if axis == dim else 1 for axis in range(len(shape))])
    return factor_of


def scatter_about(stream_key, dims, spread, most, cuts=(), held_as=jnp.bfloat16):
    array = jax.random.normal(stream_key, dims, jnp.float32) * spread
    if len(cuts) > 0:
        array = block_levels(stream_key, dims, cuts, -0.22, 0.18) * array
    return jnp.clip(array, min=-most, max=most).astype(held_as)


def setup_inputs(seed: int = 0, part: int = 0) -> dict:
    key_list = jax.random.split(jax.random.key(seed), 7)
    part_keys = jax.random.split(jax.random.fold_in(key_list[6], part), 7)
    return {
        "queries": draw_queries(jax.random.fold_in(jax.random.fold_in(key_list[6], part), 71), part),
        "keys": draw_keys(jax.random.fold_in(jax.random.fold_in(key_list[6], part), 71), part),
        "values": scatter_about(part_keys[2], (TOKENS, HEADS * HEAD_DIM), 1.0, 6.0, ((0, 16),)),
        "past_outputs": scatter_about(part_keys[3], (PAST, TOKENS, HEADS * HEAD_DIM), 1.0, 6.0, ((1, 16),)),
        "dwa_slot": jax.random.randint(key_list[4], (PAST,), 0, TABLE).astype(jnp.int32),
        "dwa_table": jnp.clip(jax.random.uniform(key_list[5], (2, TABLE), jnp.float32, 0.1, 0.6), 0.1, 0.6),
    }


def one_head(items):
    query, key_block, value_block, allowed = items
    scores = jnp.dot(query, key_block.T, preferred_element_type=jnp.float32) * (1.0 / (HEAD_DIM ** 0.5))
    scores = jnp.where(allowed, scores, -jnp.inf)
    top_score = jnp.max(scores, axis=1, keepdims=True)
    prob = jnp.exp(scores - top_score)
    total = jnp.sum(prob, axis=1, keepdims=True)
    weights = prob.astype(jnp.bfloat16)
    summed = jnp.dot(weights, value_block, preferred_element_type=jnp.float32)
    return (summed / total).astype(jnp.bfloat16)


def reference(queries, keys, values, past_outputs, dwa_slot, dwa_table):
    block_rows = N_ULY * TOK_DEV

    def arrange(field):
        return field.reshape(N_SEQ, block_rows, HEADS, HEAD_DIM)

    padding = jnp.zeros((SPAN - 1, block_rows, HEADS, HEAD_DIM), jnp.bfloat16)
    query_all = arrange(queries)
    key_padded = jnp.concatenate([padding, arrange(keys)], axis=0)
    value_padded = jnp.concatenate([padding, arrange(values)], axis=0)

    def one_block(block):
        query_block = lax.dynamic_index_in_dim(query_all, block, 0, keepdims=False)
        key_window = lax.dynamic_slice_in_dim(key_padded, block, SPAN, 0).reshape(SPAN * block_rows, HEADS, HEAD_DIM)
        value_window = lax.dynamic_slice_in_dim(value_padded, block, SPAN, 0).reshape(SPAN * block_rows, HEADS, HEAD_DIM)
        query_pos = block * block_rows + jnp.arange(block_rows, dtype=jnp.int32)
        key_pos = (block - SPAN + 1) * block_rows + jnp.arange(SPAN * block_rows, dtype=jnp.int32)
        allowed = (key_pos[None, :] <= query_pos[:, None]) & (key_pos[None, :] >= 0)
        allowed_heads = jnp.broadcast_to(allowed[None, :, :], (HEADS, block_rows, SPAN * block_rows))
        result = lax.map(one_head, (jnp.transpose(query_block, (1, 0, 2)), jnp.transpose(key_window, (1, 0, 2)), jnp.transpose(value_window, (1, 0, 2)), allowed_heads))
        return jnp.transpose(result, (1, 0, 2))

    attended = lax.map(one_block, jnp.arange(N_SEQ, dtype=jnp.int32))
    attended = attended.reshape(TOKENS, HEADS * HEAD_DIM)
    coef_in = dwa_table[0][dwa_slot]
    coef_out = dwa_table[1][dwa_slot]
    layer_in = jnp.zeros((TOKENS, HEADS * HEAD_DIM), jnp.float32)
    extra = jnp.zeros((TOKENS, HEADS * HEAD_DIM), jnp.float32)
    for index in range(PAST):
        stored = past_outputs[index].astype(jnp.float32)
        layer_in = layer_in + coef_in[index] * stored
        extra = extra + coef_out[index] * stored
    hidden = layer_in + attended.astype(jnp.float32)
    return (hidden + extra).astype(jnp.bfloat16)
```

```python
import functools
import math

import jax
import jax.numpy as jnp
from jax import lax
from jax.experimental import pallas as pl
from jax.experimental.pallas import tpu as pltpu
from jax.sharding import PartitionSpec as P

HEAD_DIM = 128
SPAN = 4
STAT = 16
MESH = pl.DeviceIdType.MESH
Q, K, V = 0, 1, 2


def from_behind(block, axis, distance):
    devices = range(lax.axis_size(axis))
    route = [(i - distance, i) for i in devices if i - distance in devices]
    return lax.ppermute(block, axis, route)


def block_update(state, query_heads, key_heads, value_heads, allowed):
    running, total, accumulated = state
    scores = jnp.einsum("qhd,khd->hqk", query_heads, key_heads, preferred_element_type=jnp.float32)
    scores = scores * (1.0 / HEAD_DIM**0.5)
    scores = jnp.where(allowed, scores, -jnp.inf)
    new_max = jnp.maximum(running, jnp.max(scores, axis=2))
    factor = jnp.exp(running - new_max)
    prob = jnp.exp(scores - new_max[:, :, None])
    total = total * factor + jnp.sum(prob, axis=2)
    weights = prob.astype(jnp.bfloat16)
    update = jnp.einsum("hqk,khd->qhd", weights, value_heads, preferred_element_type=jnp.float32)
    accumulated = accumulated * jnp.transpose(factor)[:, :, None] + update
    return (new_max, total, accumulated)


def shards(queries, keys, values, past_outputs, dwa_slot, dwa_table):
    n_uly = lax.axis_size("uly")
    n_seq = lax.axis_size("seq")
    span_size = min(4, n_seq)
    features = queries.shape[1]
    local_heads = features // n_uly // HEAD_DIM
    query_rows, key_rows, value_rows = (
        lax.all_to_all(queries, "uly", split_axis=1, concat_axis=0, tiled=True),
        lax.all_to_all(keys, "uly", split_axis=1, concat_axis=0, tiled=True),
        lax.all_to_all(values, "uly", split_axis=1, concat_axis=0, tiled=True),
    )
    row_count = query_rows.shape[0]
    split_shape = (row_count, local_heads, HEAD_DIM)
    query_heads = query_rows.reshape(split_shape)
    table_index = jnp.arange(dwa_table.shape[1])
    onehot = (dwa_slot[:, None] == table_index[None, :]).astype(jnp.float32)
    coefs = jnp.dot(onehot, jnp.transpose(dwa_table), precision=lax.Precision.HIGHEST)
    layer_in = jnp.zeros(queries.shape, jnp.float32)
    extra = jnp.zeros(queries.shape, jnp.float32)
    for index in range(past_outputs.shape[0]):
        stored = past_outputs[index].astype(jnp.float32)
        layer_in = layer_in + coefs[index, 0] * stored
        extra = extra + coefs[index, 1] * stored
    running = jnp.full((local_heads, row_count), -jnp.inf, jnp.float32)
    total = jnp.zeros((local_heads, row_count), jnp.float32)
    accumulated = jnp.zeros(split_shape, jnp.float32)
    state = (running, total, accumulated)
    causal = (jnp.arange(row_count)[:, None] >= jnp.arange(row_count)[None, :])[None, :, :]
    state = block_update(
        state, query_heads, key_rows.reshape(split_shape), value_rows.reshape(split_shape), causal
    )
    position = lax.axis_index("seq")
    current = (key_rows, value_rows)
    for offset in range(1, span_size):
        current = from_behind((current[0], current[1]), "seq", 1)
        far_keys = current[0].reshape(split_shape)
        far_values = current[1].reshape(split_shape)

        def take_block(carry, far_keys=far_keys, far_values=far_values):
            return block_update(carry, query_heads, far_keys, far_values, True)

        def keep_block(carry):
            return carry

        state = lax.cond(position >= offset, take_block, keep_block, state)
    running, total, accumulated = state
    attended = accumulated / jnp.transpose(total)[:, :, None]
    attended = attended.astype(jnp.bfloat16).reshape(row_count, local_heads * HEAD_DIM)
    returned = lax.all_to_all(attended, "uly", split_axis=0, concat_axis=1, tiled=True)
    hidden = layer_in + returned.astype(jnp.float32)
    return (hidden + extra).astype(jnp.bfloat16)


def fused_kernel(
    shape,
    slot_ref, table_ref, q_hbm, k_hbm, v_hbm, past_hbm, out_ref,
    given, past, heads, own, own_stat, part_out, part_in, att, back,
    load_sem, past_sem, plane_sem, line_sem, heads_sem, part_send, part_recv, att_sem, back_sem,
):
    n_seq, n_uly, group = shape
    tokens = given.shape[1]
    rows = n_uly * tokens
    half = rows // 2
    scale = math.log2(math.e) / HEAD_DIM**0.5
    s, t = lax.axis_index("seq"), lax.axis_index("uly")
    alone = group - 1
    shared = group - 1

    loads = [
        pltpu.make_async_copy(src, given.at[i], load_sem.at[i]) for i, src in enumerate((q_hbm, k_hbm, v_hbm))
    ]
    for load in loads:
        load.start()
    past_load = pltpu.make_async_copy(past_hbm, past, past_sem)
    past_load.start()

    barrier = pltpu.get_barrier_semaphore()
    for d in range(1, n_uly):
        pl.semaphore_signal(barrier, inc=1, device_id={"uly": lax.rem(t + d, n_uly)}, device_id_type=MESH)
    for d in range(1, n_seq):
        pl.semaphore_signal(barrier, inc=1, device_id={"seq": lax.rem(s + d, n_seq)}, device_id_type=MESH)

    @pl.when(s == 3)
    def _():
        for d in range(1, n_uly):
            pl.semaphore_signal(
                barrier, inc=1, device_id={"seq": 2, "uly": lax.rem(t + d, n_uly)}, device_id_type=MESH
            )

    pl.semaphore_wait(barrier, n_uly + n_seq - 2 + jnp.where(s == 2, n_uly - 1, 0))
    for load in loads:
        load.wait()

    def columns(uly, g):
        return pl.ds(pl.multiple_of((uly * group + g) * HEAD_DIM, HEAD_DIM), HEAD_DIM)

    my_rows = pl.ds(pl.multiple_of(t * tokens, tokens), tokens)

    def plane(kind, g, d):
        peer = lax.rem(t + d, n_uly)
        src = given.at[kind, :, columns(peer, g)]
        dst = heads.at[kind, g, s, my_rows, :]
        if d == 0:
            return pltpu.make_async_copy(src, dst, heads_sem.at[kind, g, s])
        return pltpu.make_async_remote_copy(
            src, dst, plane_sem.at[kind, g, d], heads_sem.at[kind, g, s],
            device_id={"uly": peer}, device_id_type=MESH,
        )

    def scatter(kind, g):
        for d in (*range(1, n_uly), 0):
            plane(kind, g, d).start()

    def arrived(kind, g, block):
        ref = heads.at[kind, g, block]
        pltpu.make_async_copy(ref, ref, heads_sem.at[kind, g, block]).wait()

    def line(kind, g, to, lane=0):
        ref = heads.at[kind, g, s]
        return pltpu.make_async_remote_copy(
            ref, ref, line_sem.at[kind, g, lane], heads_sem.at[kind, g, s],
            device_id={"seq": to}, device_id_type=MESH,
        )

    def partial(g, block):
        return pltpu.make_async_remote_copy(
            part_out.at[g, block - n_seq // 2], part_in.at[g],
            part_send.at[g, block - n_seq // 2], part_recv.at[g],
            device_id={"seq": block}, device_id_type=MESH,
        )

    def returning(g, lane, block, d):
        peer = lax.rem(t + d, n_uly)
        src = att.at[lane, g, pl.ds(pl.multiple_of(peer * tokens, tokens), tokens), :]
        dst = back.at[:, columns(t, g)]
        if block is None and d == 0:
            return pltpu.make_async_copy(src, dst, back_sem.at[g, t])
        where = {"uly": peer} if block is None else {"seq": block, "uly": peer}
        return pltpu.make_async_remote_copy(
            src, dst, att_sem.at[lane, g, d], back_sem.at[g, t], device_id=where, device_id_type=MESH,
        )

    def give_back(g, lane=0, block=None):
        for d in (*range(1, n_uly), 0):
            returning(g, lane, block, d).start()

    def attend(g, block, full, diagonal, finish):
        for a in range(2):
            query = heads[Q, g, block, a * half:(a + 1) * half, :]
            top = total = acc = None
            spans = [(j, rows, False) for j in full] + ([(block, (a + 1) * half, True)] if diagonal else [])
            for j, count, masked in spans:
                key = heads[K, g, j, 0:count, :]
                value = heads[V, g, j, 0:count, :]
                scores = lax.dot_general(key, query, (((1,), (1,)), ((), ())), preferred_element_type=jnp.float32)
                scores = scores * scale
                if masked:
                    key_at = lax.broadcasted_iota(jnp.int32, scores.shape, 0)
                    query_at = lax.broadcasted_iota(jnp.int32, scores.shape, 1) + a * half
                    scores = jnp.where(key_at <= query_at, scores, -jnp.inf)
                peak = jnp.max(scores, axis=0, keepdims=True)
                new_top = peak if top is None else jnp.maximum(top, peak)
                prob = jnp.exp2(scores - new_top)
                sums = jnp.sum(prob, axis=0, keepdims=True)
                update = lax.dot_general(
                    value, prob.astype(jnp.bfloat16), (((0,), (0,)), ((), ())), preferred_element_type=jnp.float32
                )
                if top is None:
                    total, acc = sums, update
                else:
                    factor = jnp.exp2(top - new_top)
                    total = total * factor + sums
                    acc = acc * factor + update
                top = new_top
            finish(slice(a * half, (a + 1) * half), top, total, acc)

    def settle(g, lane=0):
        def finish(cut, top, total, acc):
            att[lane, g, cut, :] = jnp.transpose(acc / total).astype(jnp.bfloat16)
        return finish

    def keep(g):
        def finish(cut, top, total, acc):
            own[g, :, cut] = acc
            own_stat[g, 0:1, cut] = top
            own_stat[g, 1:2, cut] = total
        return finish

    def hand_over(g, where):
        def finish(cut, top, total, acc):
            part_out[g, where, 0:HEAD_DIM, cut] = (acc / total).astype(jnp.bfloat16)
            level = top + jnp.log2(total)
            high = level.astype(jnp.bfloat16).astype(jnp.float32)
            middle = (level - high).astype(jnp.bfloat16).astype(jnp.float32)
            low = level - high - middle
            row = lax.broadcasted_iota(jnp.int32, (STAT, half), 0)
            stats = jnp.where(row == 0, high, jnp.where(row == 1, middle, jnp.where(row == 2, low, 0.0)))
            part_out[g, where, HEAD_DIM:HEAD_DIM + STAT, cut] = stats.astype(jnp.bfloat16)
        return finish

    def merge(g):
        pltpu.make_async_copy(part_in.at[g], part_in.at[g], part_recv.at[g]).wait()
        for a in range(2):
            cut = slice(a * half, (a + 1) * half)
            stats = part_in[g, HEAD_DIM:HEAD_DIM + STAT, cut].astype(jnp.float32)
            level = stats[0:1] + stats[1:2] + stats[2:3]
            top, total = own_stat[g, 0:1, cut], own_stat[g, 1:2, cut]
            new_top = jnp.maximum(top, level)
            mine, theirs = jnp.exp2(top - new_top), jnp.exp2(level - new_top)
            inverse = 1.0 / (total * mine + theirs)
            other = part_in[g, 0:HEAD_DIM, cut].astype(jnp.float32)
            both = own[g, :, cut] * (mine * inverse) + other * (theirs * inverse)
            att[0, g, cut, :] = jnp.transpose(both).astype(jnp.bfloat16)

    def each(count, body):
        def step(g, carry):
            body(g)
            return carry
        lax.fori_loop(0, count, step, 0)

    every = (alone, *range(shared))

    @pl.when(s == 0)
    def _():
        for g in every:
            scatter(K, g)
            scatter(V, g)
        for g in every:
            scatter(Q, g)
        for g in every:
            for kind in (K, V):
                arrived(kind, g, 0)
                if g == alone:
                    line(kind, g, 2, 1).start()
                else:
                    line(kind, g, 1).start()
        for kind in (K, V):
            line(kind, alone, 1).start()

        def work(g):
            arrived(Q, g, 0)
            attend(g, 0, (), True, settle(g))
            give_back(g)
        each(group, work)

    @pl.when(s == 1)
    def _():
        for g in every:
            scatter(K, g)
            scatter(V, g)
        for g in every:
            scatter(Q, g)
        for kind in (K, V):
            arrived(kind, alone, 1)
            line(kind, alone, 2).start()

        def far(g):
            for kind in (K, V):
                arrived(kind, g, 1)
                arrived(kind, g, 0)
            for block in (2, 3):
                arrived(Q, g, block)
                attend(g, block, (0, 1), False, hand_over(g, block - n_seq // 2))
                partial(g, block).start()
        each(shared, far)
        for kind in (K, V):
            arrived(kind, alone, 0)

        def near(g):
            arrived(Q, g, 1)
            attend(g, 1, (0,), True, settle(g))
            give_back(g)
        each(group, near)

    @pl.when(s == 2)
    def _():
        for g in range(shared):
            scatter(Q, g)
        for g in range(shared):
            scatter(K, g)
            scatter(V, g)
        for kind in (Q, K, V):
            scatter(kind, alone)
        for g in range(shared):
            arrived(Q, g, 2)
            line(Q, g, 1).start()
        for g in range(shared):
            for kind in (K, V):
                arrived(kind, g, 2)
                line(kind, g, 3).start()

        def near(g):
            attend(g, 2, (), True, keep(g))
        each(shared, near)
        for kind in (Q, K, V):
            arrived(kind, alone, 2)
        for kind in (K, V):
            arrived(kind, alone, 0)
            arrived(kind, alone, 1)
        attend(alone, 2, (0, 1), True, settle(alone))
        give_back(alone)
        for kind in (Q, K, V):
            arrived(kind, alone, 3)
        attend(alone, 3, (0, 1, 2), True, settle(alone, 1))
        give_back(alone, 1, 3)

        def join(g):
            merge(g)
            give_back(g)
        each(shared, join)

    @pl.when(s == 3)
    def _():
        for g in range(shared):
            scatter(Q, g)
        for kind in (Q, K, V):
            scatter(kind, alone)
        for g in range(shared):
            scatter(K, g)
            scatter(V, g)
        for g in range(shared):
            arrived(Q, g, 3)
            line(Q, g, 1).start()
        for kind in (Q, K, V):
            arrived(kind, alone, 3)
            line(kind, alone, 2).start()

        def near(g):
            for kind in (K, V):
                arrived(kind, g, 3)
                arrived(kind, g, 2)
            attend(g, 3, (2,), True, keep(g))
        each(shared, near)

        def join(g):
            merge(g)
            give_back(g)
        each(shared, join)

    past_load.wait()
    weights = [table_ref[0, slot_ref[p]] + table_ref[1, slot_ref[p]] for p in range(past.shape[0])]

    def combine(g):
        for uly in range(n_uly):
            cols = columns(uly, g)
            pltpu.make_async_copy(back.at[:, cols], back.at[:, cols], back_sem.at[g, uly]).wait()
            mixed = back[:, cols].astype(jnp.float32)
            for p, weight in enumerate(weights):
                mixed = mixed + weight * past[p, :, cols].astype(jnp.float32)
            out_ref[:, cols] = mixed.astype(out_ref.dtype)
    each(group, combine)

    for g in range(group):
        for d in range(1, n_uly):
            for kind in (Q, K, V):
                plane(kind, g, d).wait_send()

    def returned(g, lane=0, block=None):
        for d in range(0 if block is not None else 1, n_uly):
            returning(g, lane, block, d).wait_send()

    @pl.when(s == 0)
    def _():
        for g in range(group):
            for kind in (K, V):
                line(kind, g, 1).wait_send()
            returned(g)
        for kind in (K, V):
            line(kind, alone, 2, 1).wait_send()

    @pl.when(s == 1)
    def _():
        for kind in (K, V):
            line(kind, alone, 2).wait_send()
        for g in range(shared):
            for block in (2, 3):
                partial(g, block).wait_send()
        for g in range(group):
            returned(g)

    @pl.when(s == 2)
    def _():
        for g in range(shared):
            line(Q, g, 1).wait_send()
            for kind in (K, V):
                line(kind, g, 3).wait_send()
        for g in range(group):
            returned(g)
        returned(alone, 1, 3)

    @pl.when(s == 3)
    def _():
        for g in range(shared):
            line(Q, g, 1).wait_send()
            returned(g)
        for kind in (Q, K, V):
            line(kind, alone, 2).wait_send()


def fused(queries, keys, values, past_outputs, dwa_slot, dwa_table):
    n_seq, n_uly = lax.axis_size("seq"), lax.axis_size("uly")
    tokens, features = queries.shape
    group = features // n_uly // HEAD_DIM
    rows = tokens * n_uly
    stored = past_outputs.shape[0]
    bf16, f32 = jnp.bfloat16, jnp.float32
    anywhere = pl.BlockSpec(memory_space=pl.ANY)
    scalars = pl.BlockSpec(memory_space=pltpu.SMEM)
    return pl.pallas_call(
        functools.partial(fused_kernel, (n_seq, n_uly, group)),
        out_shape=jax.ShapeDtypeStruct((tokens, features), bf16),
        in_specs=[scalars, scalars, anywhere, anywhere, anywhere, anywhere],
        out_specs=pl.BlockSpec(memory_space=pltpu.VMEM),
        scratch_shapes=[
            pltpu.VMEM((3, tokens, features), bf16),
            pltpu.VMEM((stored, tokens, features), bf16),
            pltpu.VMEM((3, group, n_seq, rows, HEAD_DIM), bf16),
            pltpu.VMEM((group, HEAD_DIM, rows), f32),
            pltpu.VMEM((group, 8, rows), f32),
            pltpu.VMEM((group, 2, HEAD_DIM + STAT, rows), bf16),
            pltpu.VMEM((group, HEAD_DIM + STAT, rows), bf16),
            pltpu.VMEM((2, group, rows, HEAD_DIM), bf16),
            pltpu.VMEM((tokens, features), bf16),
            pltpu.SemaphoreType.DMA((3,)),
            pltpu.SemaphoreType.DMA,
            pltpu.SemaphoreType.DMA((3, group, n_uly)),
            pltpu.SemaphoreType.DMA((3, group, 2)),
            pltpu.SemaphoreType.DMA((3, group, n_seq)),
            pltpu.SemaphoreType.DMA((group, 2)),
            pltpu.SemaphoreType.DMA((group,)),
            pltpu.SemaphoreType.DMA((2, group, n_uly)),
            pltpu.SemaphoreType.DMA((group, n_uly)),
        ],
        compiler_params=pltpu.CompilerParams(
            collective_id=0, has_side_effects=True, vmem_limit_bytes=48 * 1024 * 1024
        ),
    )(dwa_slot, dwa_table, queries, keys, values, past_outputs)


def solution(mesh):
    body = fused if mesh.shape["seq"] == SPAN else shards
    return jax.shard_map(
        body,
        mesh=mesh,
        in_specs=(
            P(("rep", "seq", "uly"), None),
            P(("rep", "seq", "uly"), None),
            P(("rep", "seq", "uly"), None),
            P(None, ("rep", "seq", "uly"), None),
            P(),
            P(),
        ),
        out_specs=P(("rep", "seq", "uly"), None),
        check_vma=False,
    )
```

```python
import functools
import math

import jax
import jax.numpy as jnp
from jax import lax
from jax.experimental import pallas as pl
from jax.experimental.pallas import tpu as pltpu
from jax.sharding import PartitionSpec as P

HEAD_DIM = 128
SPAN = 4
STAT = 16
MESH = pl.DeviceIdType.MESH
Q, K, V = 0, 1, 2


def from_behind(block, axis, distance):
    devices = range(lax.axis_size(axis))
    route = [(i - distance, i) for i in devices if i - distance in devices]
    return lax.ppermute(block, axis, route)


def block_update(state, query_heads, key_heads, value_heads, allowed):
    running, total, accumulated = state
    scores = jnp.einsum("qhd,khd->hqk", query_heads, key_heads, preferred_element_type=jnp.float32)
    scores = scores * (1.0 / HEAD_DIM**0.5)
    scores = jnp.where(allowed, scores, -jnp.inf)
    new_max = jnp.maximum(running, jnp.max(scores, axis=2))
    factor = jnp.exp(running - new_max)
    prob = jnp.exp(scores - new_max[:, :, None])
    total = total * factor + jnp.sum(prob, axis=2)
    weights = prob.astype(jnp.bfloat16)
    update = jnp.einsum("hqk,khd->qhd", weights, value_heads, preferred_element_type=jnp.float32)
    accumulated = accumulated * jnp.transpose(factor)[:, :, None] + update
    return (new_max, total, accumulated)


def shards(queries, keys, values, past_outputs, dwa_slot, dwa_table):
    n_uly = lax.axis_size("uly")
    n_seq = lax.axis_size("seq")
    span_size = min(4, n_seq)
    features = queries.shape[1]
    local_heads = features // n_uly // HEAD_DIM
    query_rows, key_rows, value_rows = (
        lax.all_to_all(queries, "uly", split_axis=1, concat_axis=0, tiled=True),
        lax.all_to_all(keys, "uly", split_axis=1, concat_axis=0, tiled=True),
        lax.all_to_all(values, "uly", split_axis=1, concat_axis=0, tiled=True),
    )
    row_count = query_rows.shape[0]
    split_shape = (row_count, local_heads, HEAD_DIM)
    query_heads = query_rows.reshape(split_shape)
    table_index = jnp.arange(dwa_table.shape[1])
    onehot = (dwa_slot[:, None] == table_index[None, :]).astype(jnp.float32)
    coefs = jnp.dot(onehot, jnp.transpose(dwa_table), precision=lax.Precision.HIGHEST)
    layer_in = jnp.zeros(queries.shape, jnp.float32)
    extra = jnp.zeros(queries.shape, jnp.float32)
    for index in range(past_outputs.shape[0]):
        stored = past_outputs[index].astype(jnp.float32)
        layer_in = layer_in + coefs[index, 0] * stored
        extra = extra + coefs[index, 1] * stored
    running = jnp.full((local_heads, row_count), -jnp.inf, jnp.float32)
    total = jnp.zeros((local_heads, row_count), jnp.float32)
    accumulated = jnp.zeros(split_shape, jnp.float32)
    state = (running, total, accumulated)
    causal = (jnp.arange(row_count)[:, None] >= jnp.arange(row_count)[None, :])[None, :, :]
    state = block_update(
        state, query_heads, key_rows.reshape(split_shape), value_rows.reshape(split_shape), causal
    )
    position = lax.axis_index("seq")
    current = (key_rows, value_rows)
    for offset in range(1, span_size):
        current = from_behind((current[0], current[1]), "seq", 1)
        far_keys = current[0].reshape(split_shape)
        far_values = current[1].reshape(split_shape)

        def take_block(carry, far_keys=far_keys, far_values=far_values):
            return block_update(carry, query_heads, far_keys, far_values, True)

        def keep_block(carry):
            return carry

        state = lax.cond(position >= offset, take_block, keep_block, state)
    running, total, accumulated = state
    attended = accumulated / jnp.transpose(total)[:, :, None]
    attended = attended.astype(jnp.bfloat16).reshape(row_count, local_heads * HEAD_DIM)
    returned = lax.all_to_all(attended, "uly", split_axis=0, concat_axis=1, tiled=True)
    hidden = layer_in + returned.astype(jnp.float32)
    return (hidden + extra).astype(jnp.bfloat16)


def fused_kernel(
    shape,
    slot_ref, table_ref, q_hbm, k_hbm, v_hbm, past_hbm, out_ref,
    given, past, heads, own, own_stat, part_out, part_in, att, back,
    load_sem, past_sem, plane_sem, line_sem, heads_sem, part_send, part_recv, att_sem, back_sem,
):
    n_seq, n_uly, group = shape
    tokens = given.shape[1]
    rows = n_uly * tokens
    half = rows // 2
    scale = math.log2(math.e) / HEAD_DIM**0.5
    s, t = lax.axis_index("seq"), lax.axis_index("uly")
    alone = group - 1
    shared = group - 1
    guest = 0
    late, visit = group, group + 1

    loads = [
        pltpu.make_async_copy(src, given.at[i], load_sem.at[i]) for i, src in enumerate((q_hbm, k_hbm, v_hbm))
    ]
    for load in loads:
        load.start()
    past_load = pltpu.make_async_copy(past_hbm, past, past_sem)
    past_load.start()

    barrier = pltpu.get_barrier_semaphore()
    for d in range(1, n_uly):
        pl.semaphore_signal(barrier, inc=1, device_id={"uly": lax.rem(t + d, n_uly)}, device_id_type=MESH)
    for d in range(1, n_seq):
        pl.semaphore_signal(barrier, inc=1, device_id={"seq": lax.rem(s + d, n_seq)}, device_id_type=MESH)

    @pl.when(s == 3)
    def _():
        for d in range(1, n_uly):
            pl.semaphore_signal(
                barrier, inc=1, device_id={"seq": 2, "uly": lax.rem(t + d, n_uly)}, device_id_type=MESH
            )

    pl.semaphore_wait(barrier, n_uly + n_seq - 2 + jnp.where(s == 2, n_uly - 1, 0))
    for load in loads:
        load.wait()

    def columns(uly, g):
        return pl.ds(pl.multiple_of((uly * group + g) * HEAD_DIM, HEAD_DIM), HEAD_DIM)

    my_rows = pl.ds(pl.multiple_of(t * tokens, tokens), tokens)

    def plane(kind, g, d):
        peer = lax.rem(t + d, n_uly)
        src = given.at[kind, :, columns(peer, g)]
        dst = heads.at[kind, g, s, my_rows, :]
        if d == 0:
            return pltpu.make_async_copy(src, dst, heads_sem.at[kind, g, s])
        return pltpu.make_async_remote_copy(
            src, dst, plane_sem.at[kind, g, d], heads_sem.at[kind, g, s],
            device_id={"uly": peer}, device_id_type=MESH,
        )

    def scatter(kind, g):
        for d in (*range(1, n_uly), 0):
            plane(kind, g, d).start()

    def arrived(kind, g, block):
        ref = heads.at[kind, g, block]
        pltpu.make_async_copy(ref, ref, heads_sem.at[kind, g, block]).wait()

    def line(kind, g, to, lane=0, block=None):
        block = s if block is None else block
        ref = heads.at[kind, g, block]
        return pltpu.make_async_remote_copy(
            ref, ref, line_sem.at[kind, g, lane], heads_sem.at[kind, g, block],
            device_id={"seq": to}, device_id_type=MESH,
        )

    def partial(g, block, to=None, slot=None):
        slot = g if slot is None else slot
        return pltpu.make_async_remote_copy(
            part_out.at[g, block - n_seq // 2], part_in.at[slot],
            part_send.at[g, block - n_seq // 2], part_recv.at[slot],
            device_id={"seq": block if to is None else to}, device_id_type=MESH,
        )

    def returning(g, lane, block, d):
        peer = lax.rem(t + d, n_uly)
        src = att.at[lane, g, pl.ds(pl.multiple_of(peer * tokens, tokens), tokens), :]
        dst = back.at[:, columns(t, g)]
        if block is None and d == 0:
            return pltpu.make_async_copy(src, dst, back_sem.at[g, t])
        where = {"uly": peer} if block is None else {"seq": block, "uly": peer}
        return pltpu.make_async_remote_copy(
            src, dst, att_sem.at[lane, g, d], back_sem.at[g, t], device_id=where, device_id_type=MESH,
        )

    def give_back(g, lane=0, block=None):
        for d in (*range(1, n_uly), 0):
            returning(g, lane, block, d).start()

    def attend(g, block, full, diagonal, finish, resume=None):
        for a in range(2):
            query = heads[Q, g, block, a * half:(a + 1) * half, :]
            top = total = acc = None
            if resume is not None:
                cut = slice(a * half, (a + 1) * half)
                top, total, acc = own_stat[resume, 0:1, cut], own_stat[resume, 1:2, cut], own[resume, :, cut]
            spans = [(j, rows, False) for j in full] + ([(block, (a + 1) * half, True)] if diagonal else [])
            for j, count, masked in spans:
                key = heads[K, g, j, 0:count, :]
                value = heads[V, g, j, 0:count, :]
                scores = lax.dot_general(key, query, (((1,), (1,)), ((), ())), preferred_element_type=jnp.float32)
                scores = scores * scale
                if masked:
                    key_at = lax.broadcasted_iota(jnp.int32, scores.shape, 0)
                    query_at = lax.broadcasted_iota(jnp.int32, scores.shape, 1) + a * half
                    scores = jnp.where(key_at <= query_at, scores, -jnp.inf)
                peak = jnp.max(scores, axis=0, keepdims=True)
                new_top = peak if top is None else jnp.maximum(top, peak)
                prob = jnp.exp2(scores - new_top)
                sums = jnp.sum(prob, axis=0, keepdims=True)
                update = lax.dot_general(
                    value, prob.astype(jnp.bfloat16), (((0,), (0,)), ((), ())), preferred_element_type=jnp.float32
                )
                if top is None:
                    total, acc = sums, update
                else:
                    factor = jnp.exp2(top - new_top)
                    total = total * factor + sums
                    acc = acc * factor + update
                top = new_top
            finish(slice(a * half, (a + 1) * half), top, total, acc)

    def settle(g, lane=0):
        def finish(cut, top, total, acc):
            att[lane, g, cut, :] = jnp.transpose(acc / total).astype(jnp.bfloat16)
        return finish

    def keep(g):
        def finish(cut, top, total, acc):
            own[g, :, cut] = acc
            own_stat[g, 0:1, cut] = top
            own_stat[g, 1:2, cut] = total
        return finish

    def hand_over(g, where):
        def finish(cut, top, total, acc):
            part_out[g, where, 0:HEAD_DIM, cut] = (acc / total).astype(jnp.bfloat16)
            level = top + jnp.log2(total)
            high = level.astype(jnp.bfloat16).astype(jnp.float32)
            middle = (level - high).astype(jnp.bfloat16).astype(jnp.float32)
            low = level - high - middle
            row = lax.broadcasted_iota(jnp.int32, (STAT, half), 0)
            stats = jnp.where(row == 0, high, jnp.where(row == 1, middle, jnp.where(row == 2, low, 0.0)))
            part_out[g, where, HEAD_DIM:HEAD_DIM + STAT, cut] = stats.astype(jnp.bfloat16)
        return finish

    def merge(g, slot=None, lane=0):
        slot = g if slot is None else slot
        pltpu.make_async_copy(part_in.at[slot], part_in.at[slot], part_recv.at[slot]).wait()
        for a in range(2):
            cut = slice(a * half, (a + 1) * half)
            stats = part_in[slot, HEAD_DIM:HEAD_DIM + STAT, cut].astype(jnp.float32)
            level = stats[0:1] + stats[1:2] + stats[2:3]
            top, total = own_stat[slot, 0:1, cut], own_stat[slot, 1:2, cut]
            new_top = jnp.maximum(top, level)
            mine, theirs = jnp.exp2(top - new_top), jnp.exp2(level - new_top)
            inverse = 1.0 / (total * mine + theirs)
            other = part_in[slot, 0:HEAD_DIM, cut].astype(jnp.float32)
            both = own[slot, :, cut] * (mine * inverse) + other * (theirs * inverse)
            att[lane, g, cut, :] = jnp.transpose(both).astype(jnp.bfloat16)

    def each(first, count, body):
        def step(g, carry):
            body(g)
            return carry
        lax.fori_loop(first, count, step, 0)

    upward = (*range(shared - 1), alone, shared - 1)

    @pl.when(s == 0)
    def _():
        for g in upward:
            scatter(K, g)
            scatter(V, g)
        for g in upward:
            scatter(Q, g)
        for g in upward:
            for kind in (K, V):
                arrived(kind, g, 0)
                line(kind, g, 1).start()

        def work(g):
            arrived(Q, g, 0)
            attend(g, 0, (), True, settle(g))
            give_back(g)
        each(0, group, work)

    @pl.when(s == 1)
    def _():
        scatter(K, alone)
        scatter(V, alone)
        for g in range(shared):
            scatter(K, g)
            scatter(V, g)
        for g in range(group):
            scatter(Q, g)
        for kind in (K, V):
            arrived(kind, alone, 1)
            line(kind, alone, 2).start()

        def far(g, last=3, slot=None):
            for kind in (K, V):
                arrived(kind, g, 1)
                arrived(kind, g, 0)
            for block in (2, 3):
                arrived(Q, g, block)
                attend(g, block, (0, 1), False, hand_over(g, block - n_seq // 2))
                if block == 3:
                    partial(g, block, last, slot).start()
                else:
                    partial(g, block).start()
        def near(g):
            arrived(Q, g, 1)
            attend(g, 1, (0,), True, settle(g))
            give_back(g)
        if guest == shared - 1:
            for kind in (K, V):
                arrived(kind, alone, 0)
                line(kind, alone, 2, 1, 0).start()
        far(guest, 2, visit)
        each(1, shared - 1, far)
        each(0, shared - 1, near)
        if guest < shared - 1:
            for kind in (K, V):
                arrived(kind, alone, 0)
                line(kind, alone, 2, 1, 0).start()
        each(alone, group, near)
        if guest < shared - 1:
            far(shared - 1)
        each(shared - 1, shared, near)

    @pl.when(s == 2)
    def _():
        for g in range(shared):
            scatter(Q, g)
        for g in (*range(1, shared), guest):
            scatter(K, g)
            scatter(V, g)
        for kind in (Q, K, V):
            scatter(kind, alone)
        for g in range(shared):
            arrived(Q, g, 2)
            line(Q, g, 1).start()
            arrived(Q, g, 3)
            line(Q, g, 1, 1, 3).start()
            if g > 0:
                for kind in (K, V):
                    arrived(kind, g, 2)
                    line(kind, g, 3).start()
        for kind in (K, V):
            arrived(kind, guest, 2)

        def near(g):
            attend(g, 2, (), True, keep(g))
        each(0, shared, near)
        for kind in (K, V):
            arrived(kind, guest, 3)
        attend(guest, 3, (2,), True, keep(visit))

        def join(g):
            merge(g)
            give_back(g)
        join(guest)
        for kind in (K, V):
            arrived(kind, alone, 1)
        for kind in (Q, K, V):
            arrived(kind, alone, 2)
        attend(alone, 2, (1,), True, keep(alone))
        merge(guest, visit, 1)
        give_back(guest, 1, 3)
        for kind in (Q, K, V):
            arrived(kind, alone, 3)
        attend(alone, 3, (1, 2), True, keep(late))
        each(1, shared - 1, join)
        for kind in (K, V):
            arrived(kind, alone, 0)
        attend(alone, 3, (0,), False, settle(alone, 1), late)
        give_back(alone, 1, 3)
        attend(alone, 2, (0,), False, settle(alone), alone)
        give_back(alone)
        each(max(1, shared - 1), shared, join)

    @pl.when(s == 3)
    def _():
        for g in range(shared):
            scatter(Q, g)
        for kind in (K, V):
            scatter(kind, guest)
        for g in range(1, shared):
            scatter(K, g)
            scatter(V, g)
        for kind in (Q, K, V):
            scatter(kind, alone)
        for g in range(shared):
            arrived(Q, g, 3)
            line(Q, g, 2).start()
        for kind in (K, V):
            arrived(kind, guest, 3)
            line(kind, guest, 2).start()
        for kind in (Q, K, V):
            arrived(kind, alone, 3)
            line(kind, alone, 2).start()

        def near(g):
            for kind in (K, V):
                arrived(kind, g, 3)
                arrived(kind, g, 2)
            attend(g, 3, (2,), True, keep(g))
        each(1, shared, near)

        def join(g):
            merge(g)
            give_back(g)
        each(1, shared, join)

    past_load.wait()
    weights = [table_ref[0, slot_ref[p]] + table_ref[1, slot_ref[p]] for p in range(past.shape[0])]

    def combine(g):
        for uly in range(n_uly):
            cols = columns(uly, g)
            pltpu.make_async_copy(back.at[:, cols], back.at[:, cols], back_sem.at[g, uly]).wait()
            mixed = back[:, cols].astype(jnp.float32)
            for p, weight in enumerate(weights):
                mixed = mixed + weight * past[p, :, cols].astype(jnp.float32)
            out_ref[:, cols] = mixed.astype(out_ref.dtype)
    each(0, group, combine)

    for g in range(group):
        for d in range(1, n_uly):
            for kind in (Q, K, V):
                plane(kind, g, d).wait_send()

    def returned(g, lane=0, block=None):
        for d in range(0 if block is not None else 1, n_uly):
            returning(g, lane, block, d).wait_send()

    @pl.when(s == 0)
    def _():
        for g in range(group):
            for kind in (K, V):
                line(kind, g, 1).wait_send()
            returned(g)

    @pl.when(s == 1)
    def _():
        for kind in (K, V):
            line(kind, alone, 2).wait_send()
            line(kind, alone, 2, 1, 0).wait_send()
        for g in range(shared):
            for block in (2, 3):
                partial(g, block).wait_send()
        for g in range(group):
            returned(g)

    @pl.when(s == 2)
    def _():
        for g in range(shared):
            line(Q, g, 1).wait_send()
            line(Q, g, 1, 1, 3).wait_send()
        for g in range(1, shared):
            for kind in (K, V):
                line(kind, g, 3).wait_send()
        for g in range(group):
            returned(g)
        for g in (guest, alone):
            returned(g, 1, 3)

    @pl.when(s == 3)
    def _():
        for g in range(shared):
            line(Q, g, 2).wait_send()
        for kind in (K, V):
            line(kind, guest, 2).wait_send()
        for g in range(1, shared):
            returned(g)
        for kind in (Q, K, V):
            line(kind, alone, 2).wait_send()


def fused(queries, keys, values, past_outputs, dwa_slot, dwa_table):
    n_seq, n_uly = lax.axis_size("seq"), lax.axis_size("uly")
    tokens, features = queries.shape
    group = features // n_uly // HEAD_DIM
    rows = tokens * n_uly
    stored = past_outputs.shape[0]
    bf16, f32 = jnp.bfloat16, jnp.float32
    anywhere = pl.BlockSpec(memory_space=pl.ANY)
    scalars = pl.BlockSpec(memory_space=pltpu.SMEM)
    return pl.pallas_call(
        functools.partial(fused_kernel, (n_seq, n_uly, group)),
        out_shape=jax.ShapeDtypeStruct((tokens, features), bf16),
        in_specs=[scalars, scalars, anywhere, anywhere, anywhere, anywhere],
        out_specs=pl.BlockSpec(memory_space=pltpu.VMEM),
        scratch_shapes=[
            pltpu.VMEM((3, tokens, features), bf16),
            pltpu.VMEM((stored, tokens, features), bf16),
            pltpu.VMEM((3, group, n_seq, rows, HEAD_DIM), bf16),
            pltpu.VMEM((group + 2, HEAD_DIM, rows), f32),
            pltpu.VMEM((group + 2, 8, rows), f32),
            pltpu.VMEM((group, 2, HEAD_DIM + STAT, rows), bf16),
            pltpu.VMEM((group + 2, HEAD_DIM + STAT, rows), bf16),
            pltpu.VMEM((2, group, rows, HEAD_DIM), bf16),
            pltpu.VMEM((tokens, features), bf16),
            pltpu.SemaphoreType.DMA((3,)),
            pltpu.SemaphoreType.DMA,
            pltpu.SemaphoreType.DMA((3, group, n_uly)),
            pltpu.SemaphoreType.DMA((3, group, 2)),
            pltpu.SemaphoreType.DMA((3, group, n_seq)),
            pltpu.SemaphoreType.DMA((group, 2)),
            pltpu.SemaphoreType.DMA((group + 2,)),
            pltpu.SemaphoreType.DMA((2, group, n_uly)),
            pltpu.SemaphoreType.DMA((group, n_uly)),
        ],
        compiler_params=pltpu.CompilerParams(
            collective_id=0, has_side_effects=True, vmem_limit_bytes=62 * 1024 * 1024
        ),
    )(dwa_slot, dwa_table, queries, keys, values, past_outputs)


def solution(mesh):
    def body(queries, *rest):
        heads_here = queries.shape[1] // HEAD_DIM // mesh.shape["uly"]
        fits = mesh.shape["seq"] == SPAN and heads_here >= 2
        return (fused if fits else shards)(queries, *rest)

    return jax.shard_map(
        body,
        mesh=mesh,
        in_specs=(
            P(("rep", "seq", "uly"), None),
            P(("rep", "seq", "uly"), None),
            P(("rep", "seq", "uly"), None),
            P(None, ("rep", "seq", "uly"), None),
            P(),
            P(),
        ),
        out_specs=P(("rep", "seq", "uly"), None),
        check_vma=False,
    )
```

```python
import functools
import math

import jax
import jax.numpy as jnp
from jax import lax
from jax.experimental import pallas as pl
from jax.experimental.pallas import tpu as pltpu
from jax.sharding import PartitionSpec as P

HEAD_DIM = 128
SPAN = 4
STAT = 16
MESH = pl.DeviceIdType.MESH
Q, K, V = 0, 1, 2


def from_behind(block, axis, distance):
    devices = range(lax.axis_size(axis))
    route = [(i - distance, i) for i in devices if i - distance in devices]
    return lax.ppermute(block, axis, route)


def block_update(state, query_heads, key_heads, value_heads, allowed):
    running, total, accumulated = state
    scores = jnp.einsum("qhd,khd->hqk", query_heads, key_heads, preferred_element_type=jnp.float32)
    scores = scores * (1.0 / HEAD_DIM**0.5)
    scores = jnp.where(allowed, scores, -jnp.inf)
    new_max = jnp.maximum(running, jnp.max(scores, axis=2))
    factor = jnp.exp(running - new_max)
    prob = jnp.exp(scores - new_max[:, :, None])
    total = total * factor + jnp.sum(prob, axis=2)
    weights = prob.astype(jnp.bfloat16)
    update = jnp.einsum("hqk,khd->qhd", weights, value_heads, preferred_element_type=jnp.float32)
    accumulated = accumulated * jnp.transpose(factor)[:, :, None] + update
    return (new_max, total, accumulated)


def shards(queries, keys, values, past_outputs, dwa_slot, dwa_table):
    n_uly = lax.axis_size("uly")
    n_seq = lax.axis_size("seq")
    span_size = min(4, n_seq)
    features = queries.shape[1]
    local_heads = features // n_uly // HEAD_DIM
    query_rows, key_rows, value_rows = (
        lax.all_to_all(queries, "uly", split_axis=1, concat_axis=0, tiled=True),
        lax.all_to_all(keys, "uly", split_axis=1, concat_axis=0, tiled=True),
        lax.all_to_all(values, "uly", split_axis=1, concat_axis=0, tiled=True),
    )
    row_count = query_rows.shape[0]
    split_shape = (row_count, local_heads, HEAD_DIM)
    query_heads = query_rows.reshape(split_shape)
    table_index = jnp.arange(dwa_table.shape[1])
    onehot = (dwa_slot[:, None] == table_index[None, :]).astype(jnp.float32)
    coefs = jnp.dot(onehot, jnp.transpose(dwa_table), precision=lax.Precision.HIGHEST)
    layer_in = jnp.zeros(queries.shape, jnp.float32)
    extra = jnp.zeros(queries.shape, jnp.float32)
    for index in range(past_outputs.shape[0]):
        stored = past_outputs[index].astype(jnp.float32)
        layer_in = layer_in + coefs[index, 0] * stored
        extra = extra + coefs[index, 1] * stored
    running = jnp.full((local_heads, row_count), -jnp.inf, jnp.float32)
    total = jnp.zeros((local_heads, row_count), jnp.float32)
    accumulated = jnp.zeros(split_shape, jnp.float32)
    state = (running, total, accumulated)
    causal = (jnp.arange(row_count)[:, None] >= jnp.arange(row_count)[None, :])[None, :, :]
    state = block_update(
        state, query_heads, key_rows.reshape(split_shape), value_rows.reshape(split_shape), causal
    )
    position = lax.axis_index("seq")
    current = (key_rows, value_rows)
    for offset in range(1, span_size):
        current = from_behind((current[0], current[1]), "seq", 1)
        far_keys = current[0].reshape(split_shape)
        far_values = current[1].reshape(split_shape)

        def take_block(carry, far_keys=far_keys, far_values=far_values):
            return block_update(carry, query_heads, far_keys, far_values, True)

        def keep_block(carry):
            return carry

        state = lax.cond(position >= offset, take_block, keep_block, state)
    running, total, accumulated = state
    attended = accumulated / jnp.transpose(total)[:, :, None]
    attended = attended.astype(jnp.bfloat16).reshape(row_count, local_heads * HEAD_DIM)
    returned = lax.all_to_all(attended, "uly", split_axis=0, concat_axis=1, tiled=True)
    hidden = layer_in + returned.astype(jnp.float32)
    return (hidden + extra).astype(jnp.bfloat16)


def fused_kernel(
    shape,
    slot_ref, table_ref, q_hbm, k_hbm, v_hbm, past_hbm, out_ref,
    given, past, heads, own, own_stat, part_out, part_in, att, back,
    load_sem, past_sem, plane_sem, line_sem, heads_sem, part_send, part_recv, att_sem, back_sem,
):
    n_seq, n_uly, group = shape
    tokens = given.shape[1]
    rows = n_uly * tokens
    half = rows // 2
    scale = math.log2(math.e) / HEAD_DIM**0.5
    s, t = lax.axis_index("seq"), lax.axis_index("uly")
    alone = group - 1
    shared = group - 1
    guest = 0
    late, visit = group, group + 1

    loads = [
        pltpu.make_async_copy(src, given.at[i], load_sem.at[i]) for i, src in enumerate((q_hbm, k_hbm, v_hbm))
    ]
    for load in loads:
        load.start()
    past_load = pltpu.make_async_copy(past_hbm, past, past_sem)
    past_load.start()

    barrier = pltpu.get_barrier_semaphore()
    for d in range(1, n_uly):
        pl.semaphore_signal(barrier, inc=1, device_id={"uly": lax.rem(t + d, n_uly)}, device_id_type=MESH)
    for d in range(1, n_seq):
        pl.semaphore_signal(barrier, inc=1, device_id={"seq": lax.rem(s + d, n_seq)}, device_id_type=MESH)

    @pl.when(s == 3)
    def _():
        for d in range(1, n_uly):
            pl.semaphore_signal(
                barrier, inc=1, device_id={"seq": 2, "uly": lax.rem(t + d, n_uly)}, device_id_type=MESH
            )

    pl.semaphore_wait(barrier, n_uly + n_seq - 2 + jnp.where(s == 2, n_uly - 1, 0))
    for load in loads:
        load.wait()

    def columns(uly, g):
        return pl.ds(pl.multiple_of((uly * group + g) * HEAD_DIM, HEAD_DIM), HEAD_DIM)

    my_rows = pl.ds(pl.multiple_of(t * tokens, tokens), tokens)

    def plane(kind, g, d):
        peer = lax.rem(t + d, n_uly)
        src = given.at[kind, :, columns(peer, g)]
        dst = heads.at[kind, g, s, my_rows, :]
        if d == 0:
            return pltpu.make_async_copy(src, dst, heads_sem.at[kind, g, s])
        return pltpu.make_async_remote_copy(
            src, dst, plane_sem.at[kind, g, d], heads_sem.at[kind, g, s],
            device_id={"uly": peer}, device_id_type=MESH,
        )

    def scatter(kind, g):
        for d in (*range(1, n_uly), 0):
            plane(kind, g, d).start()

    def arrived(kind, g, block):
        ref = heads.at[kind, g, block]
        pltpu.make_async_copy(ref, ref, heads_sem.at[kind, g, block]).wait()

    def line(kind, g, to, lane=0, block=None):
        block = s if block is None else block
        ref = heads.at[kind, g, block]
        return pltpu.make_async_remote_copy(
            ref, ref, line_sem.at[kind, g, lane], heads_sem.at[kind, g, block],
            device_id={"seq": to}, device_id_type=MESH,
        )

    def partial(g, block, to=None, slot=None):
        slot = g if slot is None else slot
        return pltpu.make_async_remote_copy(
            part_out.at[g, block - n_seq // 2], part_in.at[slot],
            part_send.at[g, block - n_seq // 2], part_recv.at[slot],
            device_id={"seq": block if to is None else to}, device_id_type=MESH,
        )

    def returning(g, lane, block, d):
        peer = lax.rem(t + d, n_uly)
        src = att.at[lane, g, pl.ds(pl.multiple_of(peer * tokens, tokens), tokens), :]
        dst = back.at[:, columns(t, g)]
        if block is None and d == 0:
            return pltpu.make_async_copy(src, dst, back_sem.at[g, t])
        where = {"uly": peer} if block is None else {"seq": block, "uly": peer}
        return pltpu.make_async_remote_copy(
            src, dst, att_sem.at[lane, g, d], back_sem.at[g, t], device_id=where, device_id_type=MESH,
        )

    def give_back(g, lane=0, block=None):
        for d in (*range(1, n_uly), 0):
            returning(g, lane, block, d).start()

    def attend(g, block, full, diagonal, finish, resume=None):
        for a in range(2):
            query = heads[Q, g, block, a * half:(a + 1) * half, :]
            top = total = acc = None
            if resume is not None:
                cut = slice(a * half, (a + 1) * half)
                top, total, acc = own_stat[resume, 0:1, cut], own_stat[resume, 1:2, cut], own[resume, :, cut]
            spans = [(j, rows, False) for j in full] + ([(block, (a + 1) * half, True)] if diagonal else [])
            for j, count, masked in spans:
                key = heads[K, g, j, 0:count, :]
                value = heads[V, g, j, 0:count, :]
                scores = lax.dot_general(key, query, (((1,), (1,)), ((), ())), preferred_element_type=jnp.float32)
                scores = scores * scale
                if masked:
                    key_at = lax.broadcasted_iota(jnp.int32, scores.shape, 0)
                    query_at = lax.broadcasted_iota(jnp.int32, scores.shape, 1) + a * half
                    scores = jnp.where(key_at <= query_at, scores, -jnp.inf)
                peak = jnp.max(scores, axis=0, keepdims=True)
                new_top = peak if top is None else jnp.maximum(top, peak)
                prob = jnp.exp2(scores - new_top)
                sums = jnp.sum(prob, axis=0, keepdims=True)
                update = lax.dot_general(
                    value, prob.astype(jnp.bfloat16), (((0,), (0,)), ((), ())), preferred_element_type=jnp.float32
                )
                if top is None:
                    total, acc = sums, update
                else:
                    factor = jnp.exp2(top - new_top)
                    total = total * factor + sums
                    acc = acc * factor + update
                top = new_top
            finish(slice(a * half, (a + 1) * half), top, total, acc)

    def settle(g, lane=0):
        def finish(cut, top, total, acc):
            att[lane, g, cut, :] = jnp.transpose(acc / total).astype(jnp.bfloat16)
        return finish

    def keep(g):
        def finish(cut, top, total, acc):
            own[g, :, cut] = acc
            own_stat[g, 0:1, cut] = top
            own_stat[g, 1:2, cut] = total
        return finish

    def hand_over(g, where):
        def finish(cut, top, total, acc):
            part_out[g, where, 0:HEAD_DIM, cut] = (acc / total).astype(jnp.bfloat16)
            level = top + jnp.log2(total)
            high = level.astype(jnp.bfloat16).astype(jnp.float32)
            middle = (level - high).astype(jnp.bfloat16).astype(jnp.float32)
            low = level - high - middle
            row = lax.broadcasted_iota(jnp.int32, (STAT, half), 0)
            stats = jnp.where(row == 0, high, jnp.where(row == 1, middle, jnp.where(row == 2, low, 0.0)))
            part_out[g, where, HEAD_DIM:HEAD_DIM + STAT, cut] = stats.astype(jnp.bfloat16)
        return finish

    def merge(g, slot=None, lane=0):
        slot = g if slot is None else slot
        pltpu.make_async_copy(part_in.at[slot], part_in.at[slot], part_recv.at[slot]).wait()
        for a in range(2):
            cut = slice(a * half, (a + 1) * half)
            stats = part_in[slot, HEAD_DIM:HEAD_DIM + STAT, cut].astype(jnp.float32)
            level = stats[0:1] + stats[1:2] + stats[2:3]
            top, total = own_stat[slot, 0:1, cut], own_stat[slot, 1:2, cut]
            new_top = jnp.maximum(top, level)
            mine, theirs = jnp.exp2(top - new_top), jnp.exp2(level - new_top)
            inverse = 1.0 / (total * mine + theirs)
            other = part_in[slot, 0:HEAD_DIM, cut].astype(jnp.float32)
            both = own[slot, :, cut] * (mine * inverse) + other * (theirs * inverse)
            att[lane, g, cut, :] = jnp.transpose(both).astype(jnp.bfloat16)

    def each(first, count, body):
        def step(g, carry):
            body(g)
            return carry
        lax.fori_loop(first, count, step, 0)

    upward = (*range(shared - 1), alone, shared - 1)

    @pl.when(s == 0)
    def _():
        for g in upward:
            scatter(K, g)
            scatter(V, g)
        for g in upward:
            scatter(Q, g)
        for g in upward:
            for kind in (K, V):
                arrived(kind, g, 0)
                line(kind, g, 1).start()

        def work(g):
            arrived(Q, g, 0)
            attend(g, 0, (), True, settle(g))
            give_back(g)
        each(0, group, work)

    @pl.when(s == 1)
    def _():
        scatter(K, alone)
        scatter(V, alone)
        for g in range(shared):
            scatter(K, g)
            scatter(V, g)
        for g in range(group):
            scatter(Q, g)
        for kind in (K, V):
            arrived(kind, alone, 1)
            line(kind, alone, 2).start()

        def far(g, last=3, slot=None):
            for kind in (K, V):
                arrived(kind, g, 1)
                arrived(kind, g, 0)
            for block in (3, 2):
                arrived(Q, g, block)
                attend(g, block, (0, 1), False, hand_over(g, block - n_seq // 2))
                if block == 3:
                    partial(g, block, last, slot).start()
                else:
                    partial(g, block).start()
        def near(g):
            arrived(Q, g, 1)
            attend(g, 1, (0,), True, settle(g))
            give_back(g)
        if guest == shared - 1:
            for kind in (K, V):
                arrived(kind, alone, 0)
                line(kind, alone, 2, 1, 0).start()
        far(guest, 2, visit)
        each(1, shared - 1, far)
        each(0, shared - 1, near)
        if guest < shared - 1:
            for kind in (K, V):
                arrived(kind, alone, 0)
                line(kind, alone, 2, 1, 0).start()
        each(alone, group, near)
        if guest < shared - 1:
            far(shared - 1)
        each(shared - 1, shared, near)

    @pl.when(s == 2)
    def _():
        for g in range(shared):
            scatter(Q, g)
        for g in (*range(1, shared), guest):
            scatter(K, g)
            scatter(V, g)
        for kind in (Q, K, V):
            scatter(kind, alone)
        for g in range(shared):
            arrived(Q, g, 2)
            line(Q, g, 1).start()
            arrived(Q, g, 3)
            line(Q, g, 1, 1, 3).start()
            if g > 0:
                for kind in (K, V):
                    arrived(kind, g, 2)
                    line(kind, g, 3).start()
        for kind in (K, V):
            arrived(kind, guest, 2)

        def near(g):
            attend(g, 2, (), True, keep(g))
        each(0, shared, near)
        for kind in (K, V):
            arrived(kind, guest, 3)
        attend(guest, 3, (2,), True, keep(visit))

        def join(g):
            merge(g)
            give_back(g)
        join(guest)
        for kind in (K, V):
            arrived(kind, alone, 1)
        for kind in (Q, K, V):
            arrived(kind, alone, 2)
        attend(alone, 2, (1,), True, keep(alone))
        merge(guest, visit, 1)
        give_back(guest, 1, 3)
        for kind in (Q, K, V):
            arrived(kind, alone, 3)
        attend(alone, 3, (1, 2), True, keep(late))
        each(1, shared - 1, join)
        for kind in (K, V):
            arrived(kind, alone, 0)
        attend(alone, 3, (0,), False, settle(alone, 1), late)
        give_back(alone, 1, 3)
        attend(alone, 2, (0,), False, settle(alone), alone)
        give_back(alone)
        each(max(1, shared - 1), shared, join)

    @pl.when(s == 3)
    def _():
        for g in range(shared):
            scatter(Q, g)
        for kind in (K, V):
            scatter(kind, guest)
        for g in range(1, shared):
            scatter(K, g)
            scatter(V, g)
        for kind in (Q, K, V):
            scatter(kind, alone)
        for g in range(shared):
            arrived(Q, g, 3)
            line(Q, g, 2).start()
        for kind in (K, V):
            arrived(kind, guest, 3)
            line(kind, guest, 2).start()
        for kind in (Q, K, V):
            arrived(kind, alone, 3)
            line(kind, alone, 2).start()

        def near(g):
            for kind in (K, V):
                arrived(kind, g, 3)
                arrived(kind, g, 2)
            attend(g, 3, (2,), True, keep(g))
        each(1, shared, near)

        def join(g):
            merge(g)
            give_back(g)
        each(1, shared, join)

    past_load.wait()
    weights = [table_ref[0, slot_ref[p]] + table_ref[1, slot_ref[p]] for p in range(past.shape[0])]

    def combine(g):
        for uly in range(n_uly):
            cols = columns(uly, g)
            pltpu.make_async_copy(back.at[:, cols], back.at[:, cols], back_sem.at[g, uly]).wait()
            mixed = back[:, cols].astype(jnp.float32)
            for p, weight in enumerate(weights):
                mixed = mixed + weight * past[p, :, cols].astype(jnp.float32)
            out_ref[:, cols] = mixed.astype(out_ref.dtype)
    each(0, shared - 1, combine)
    each(alone, group, combine)
    each(shared - 1, shared, combine)

    for g in range(group):
        for d in range(1, n_uly):
            for kind in (Q, K, V):
                plane(kind, g, d).wait_send()

    def returned(g, lane=0, block=None):
        for d in range(0 if block is not None else 1, n_uly):
            returning(g, lane, block, d).wait_send()

    @pl.when(s == 0)
    def _():
        for g in range(group):
            for kind in (K, V):
                line(kind, g, 1).wait_send()
            returned(g)

    @pl.when(s == 1)
    def _():
        for kind in (K, V):
            line(kind, alone, 2).wait_send()
            line(kind, alone, 2, 1, 0).wait_send()
        for g in range(shared):
            for block in (2, 3):
                partial(g, block).wait_send()
        for g in range(group):
            returned(g)

    @pl.when(s == 2)
    def _():
        for g in range(shared):
            line(Q, g, 1).wait_send()
            line(Q, g, 1, 1, 3).wait_send()
        for g in range(1, shared):
            for kind in (K, V):
                line(kind, g, 3).wait_send()
        for g in range(group):
            returned(g)
        for g in (guest, alone):
            returned(g, 1, 3)

    @pl.when(s == 3)
    def _():
        for g in range(shared):
            line(Q, g, 2).wait_send()
        for kind in (K, V):
            line(kind, guest, 2).wait_send()
        for g in range(1, shared):
            returned(g)
        for kind in (Q, K, V):
            line(kind, alone, 2).wait_send()


def fused(queries, keys, values, past_outputs, dwa_slot, dwa_table):
    n_seq, n_uly = lax.axis_size("seq"), lax.axis_size("uly")
    tokens, features = queries.shape
    group = features // n_uly // HEAD_DIM
    rows = tokens * n_uly
    stored = past_outputs.shape[0]
    bf16, f32 = jnp.bfloat16, jnp.float32
    anywhere = pl.BlockSpec(memory_space=pl.ANY)
    scalars = pl.BlockSpec(memory_space=pltpu.SMEM)
    return pl.pallas_call(
        functools.partial(fused_kernel, (n_seq, n_uly, group)),
        out_shape=jax.ShapeDtypeStruct((tokens, features), bf16),
        in_specs=[scalars, scalars, anywhere, anywhere, anywhere, anywhere],
        out_specs=pl.BlockSpec(memory_space=pltpu.VMEM),
        scratch_shapes=[
            pltpu.VMEM((3, tokens, features), bf16),
            pltpu.VMEM((stored, tokens, features), bf16),
            pltpu.VMEM((3, group, n_seq, rows, HEAD_DIM), bf16),
            pltpu.VMEM((group + 2, HEAD_DIM, rows), f32),
            pltpu.VMEM((group + 2, 8, rows), f32),
            pltpu.VMEM((group, 2, HEAD_DIM + STAT, rows), bf16),
            pltpu.VMEM((group + 2, HEAD_DIM + STAT, rows), bf16),
            pltpu.VMEM((2, group, rows, HEAD_DIM), bf16),
            pltpu.VMEM((tokens, features), bf16),
            pltpu.SemaphoreType.DMA((3,)),
            pltpu.SemaphoreType.DMA,
            pltpu.SemaphoreType.DMA((3, group, n_uly)),
            pltpu.SemaphoreType.DMA((3, group, 2)),
            pltpu.SemaphoreType.DMA((3, group, n_seq)),
            pltpu.SemaphoreType.DMA((group, 2)),
            pltpu.SemaphoreType.DMA((group + 2,)),
            pltpu.SemaphoreType.DMA((2, group, n_uly)),
            pltpu.SemaphoreType.DMA((group, n_uly)),
        ],
        compiler_params=pltpu.CompilerParams(
            collective_id=0, has_side_effects=True, vmem_limit_bytes=62 * 1024 * 1024
        ),
    )(dwa_slot, dwa_table, queries, keys, values, past_outputs)


def solution(mesh):
    def body(queries, *rest):
        heads_here = queries.shape[1] // HEAD_DIM // mesh.shape["uly"]
        fits = mesh.shape["seq"] == SPAN and heads_here >= 2
        return (fused if fits else shards)(queries, *rest)

    return jax.shard_map(
        body,
        mesh=mesh,
        in_specs=(
            P(("rep", "seq", "uly"), None),
            P(("rep", "seq", "uly"), None),
            P(("rep", "seq", "uly"), None),
            P(None, ("rep", "seq", "uly"), None),
            P(),
            P(),
        ),
        out_specs=P(("rep", "seq", "uly"), None),
        check_vma=False,
    )
```
